768 devices in a mesh: dp: 96 (over z, x, core), mp: 8 (over y).
Axes of the slice: x: 4, y: 8, z: 12, core: 2. Of those that a mesh axis runs over, the one named last changes fastest.
Arguments:
- vision_rows: bfloat16 [24576, 1024], P('dp'), may hold values from -6 to 6
- image_count: int32 [768], P('dp'), may hold values from 0 to 4
- proj_flat: bfloat16 [36864, 128], P(('dp', 'mp')), may hold values from -0.1875 to 0.1875
- text_embeds: bfloat16 [73728, 4096], P(('dp', 'mp')), may hold values from -6 to 6
- norm_gain: float32 [4096], replicated, may hold values from 0.1 to 1.9
- q_weight: bfloat16 [4096, 4096], P(None, 'mp'), may hold values from -0.09375 to 0.09375
- q_grad: bfloat16 [98304, 4096], P('dp', 'mp'), may hold values from -6 to 6
Outputs:
- text_grad: bfloat16 [73728, 4096], P(('dp', 'mp'))
- proj_grad: float32 [36864, 128], P(('dp', 'mp'))
The draws below stay inside these ranges and needn't reach their ends.
Inputs may be any that keep to these rules, and one draw needn't show every extreme that they name: Slot s of device k holds an image when s < image_count[k]; other slots are padding.
All inputs are finite; a program needn't handle non-finite values.
Results may differ from the reference program's by a relative error of at most 0.014.
Values may be sent and summed in bfloat16 or wider, within the bound.
No kernel may reach another device: no remote copies, remote signals or barrier semaphores. Data moves between devices by JAX's collectives and lax.ppermute only.
A program may use at most 64 MiB of HBM per device.

```python
import jax
import jax.numpy as jnp
from jax import lax

D = 4096
ENC = 1024
IMG_MAX = 4
PATCH = 8
TEXT_DEV = 96
IMG_ROWS = 32
ROWS_DEV = 128
PROJ_ROWS = 48
N_DP = 96
N_MP = 8


def plant(drawn, own_key, least, largest):
    longest = drawn.shape.index(max(drawn.shape))
    spots = []
    for shift in (0, 1):
        where = [jax.random.randint(jax.random.fold_in(own_key, axis), (), 0, length) for axis, length in enumerate(drawn.shape)]
        where[longest] = (where[longest] + shift) % drawn.shape[longest]
        spots.append(tuple(where))
    return drawn.at[spots[0]].set(least).at[spots[1]].set(largest)


def block_scale(key, extent, cuts, smallest, high):
    level = 1.0
    for position, blocks in cuts:
        heights = jax.random.uniform(jax.random.fold_in(jax.random.fold_in(key, 6), position), (blocks,), jnp.float32, smallest / len(cuts), high / len(cuts))
        level = level * jnp.repeat(jnp.exp(heights), extent[position] // blocks).reshape((-1,) + (1,) * (len(extent) - 1 - position))
    return level


def bell_draw(own_key, dims, deviation, most, split=(), kind=jnp.bfloat16):
    gain = block_scale(own_key, dims, split, -0.22, 0.18) if split else 1.0
    array = jax.random.normal(own_key, dims, jnp.float32) * deviation * gain
    return jnp.minimum(jnp.maximum(array, -most), most).astype(kind)


def setup_inputs(seed: int = 0) -> dict:
    streams_of = jax.random.split(jax.random.key(seed), 8)
    vision_rows = bell_draw(streams_of[0], (N_DP * N_MP * IMG_ROWS, ENC), 1.0, 6.0, ((0, 96),))
    image_count = plant(jax.random.randint(streams_of[1], (N_DP * N_MP,), 0, IMG_MAX + 1), jax.random.fold_in(streams_of[1], 1), 0, IMG_MAX).astype(jnp.int32)
    proj_flat = bell_draw(streams_of[2], (N_DP * N_MP * PROJ_ROWS, 128), ENC ** -0.5, 0.1875, ((0, 768),))
    text_embeds = bell_draw(streams_of[3], (N_DP * N_MP * TEXT_DEV, D), 1.0, 6.0, ((0, 768),))
    norm_gain = jnp.clip(1.0 + 0.18 * jax.random.normal(streams_of[4], (D,), jnp.float32), 0.1, 1.9)
    q_weight = bell_draw(streams_of[5], (D, D), D ** -0.5, 0.09375, ((1, 8),))
    q_grad = bell_draw(streams_of[6], (N_DP * N_MP * ROWS_DEV, D), 1.0, 6.0, ((0, 96), (1, 8)))
    return {"vision_rows": vision_rows, "image_count": image_count, "proj_flat": proj_flat, "text_embeds": text_embeds, "norm_gain": norm_gain, "q_weight": q_weight, "q_grad": q_grad}


norm_eps = 1e-05

def reference(vision_rows, image_count, proj_flat, text_embeds, norm_gain, q_weight, q_grad):
    block_cols = D // N_MP
    used_count = ENC * block_cols
    stored = proj_flat.reshape(N_DP, N_MP, PROJ_ROWS * 128).transpose(1, 0, 2)
    stored = stored.reshape(N_MP, N_DP * PROJ_ROWS * 128)[:, :used_count]
    proj_weight = stored.reshape(N_MP, ENC, block_cols).transpose(1, 0, 2).reshape(ENC, D)
    image_embed = jnp.dot(vision_rows, proj_weight, preferred_element_type=jnp.float32).astype(jnp.bfloat16)
    image_blocks = image_embed.reshape(N_DP * N_MP, IMG_ROWS, D)
    text_blocks = text_embeds.reshape(N_DP * N_MP, TEXT_DEV, D)
    decoder_in = jnp.concatenate([image_blocks, text_blocks], axis=1).reshape(-1, D)
    inputs = decoder_in.astype(jnp.float32)
    inv_rms = lax.rsqrt(lax.optimization_barrier(jnp.mean(inputs * inputs, axis=-1, keepdims=True)) + norm_eps)
    norm_grad = jnp.zeros(inputs.shape, jnp.float32)
    for member in range(N_MP):
        left = q_grad[:, member * block_cols:(member + 1) * block_cols]
        right = q_weight[:, member * block_cols:(member + 1) * block_cols]
        term = jnp.dot(left, right.T, preferred_element_type=jnp.float32).astype(jnp.bfloat16)
        term = lax.optimization_barrier(term)
        norm_grad = norm_grad + term.astype(jnp.float32)
    scaled = norm_gain[None, :] * norm_grad
    inner_mean = lax.optimization_barrier(jnp.mean(scaled * inputs, axis=-1, keepdims=True))
    input_grad = inv_rms * scaled - inputs * inv_rms ** 3 * inner_mean
    grad_blocks = input_grad.reshape(N_DP * N_MP, ROWS_DEV, D)
    text_grad = grad_blocks[:, IMG_ROWS:, :].reshape(-1, D).astype(jnp.bfloat16)
    live_slots = jnp.arange(IMG_MAX, dtype=jnp.int32)[None, :] < image_count[:, None]
    live_rows = jnp.repeat(live_slots, PATCH, axis=1)
    image_grad = jnp.where(live_rows[:, :, None], grad_blocks[:, :IMG_ROWS, :], 0.0)
    image_grad = image_grad.reshape(-1, D).astype(jnp.bfloat16)
    grad_scale = 1.0 / jnp.sqrt(jnp.float32(N_DP * N_MP * IMG_ROWS))
    proj_full = jnp.dot(vision_rows.T, image_grad, preferred_element_type=jnp.float32) * grad_scale
    flat_blocks = proj_full.reshape(ENC, N_MP, block_cols).transpose(1, 0, 2).reshape(N_MP, used_count)
    flat_blocks = jnp.pad(flat_blocks, ((0, 0), (0, N_DP * PROJ_ROWS * 128 - used_count)))
    proj_grad = flat_blocks.reshape(N_MP, N_DP, PROJ_ROWS * 128).transpose(1, 0, 2)
    proj_grad = proj_grad.reshape(N_DP * N_MP * PROJ_ROWS, 128)
    return (text_grad, proj_grad)
```

```python
import jax
import jax.numpy as jnp
from jax import lax
from jax.sharding import Mesh
from jax.sharding import PartitionSpec as P

IMG_MAX = 4
PATCH = 8
DP = ("z", "x", "c")
DP_MP = ("z", "x", "c", "y")

norm_eps = 1e-05


def spread(block, axis):
    n = lax.axis_size(axis)
    copies = jnp.broadcast_to(block[None], (n, *block.shape))
    return lax.all_to_all(copies, axis, split_axis=0, concat_axis=0, tiled=True)


def summed(blocks, axis):
    parts = lax.all_to_all(
        blocks.astype(jnp.bfloat16), axis, split_axis=0, concat_axis=0, tiled=True
    )
    return jnp.sum(parts.astype(jnp.float32), axis=0)


def contract_last(left, right):
    return lax.dot_general(
        left, right, (((1,), (1,)), ((), ())), preferred_element_type=jnp.float32
    )


def body(vision_rows, image_count, proj_flat, text_embeds, norm_gain, q_weight, q_grad):
    groups = lax.axis_size("y")
    nz, nx, nc = (lax.axis_size(a) for a in DP)
    shards = nz * nx * nc
    enc_width = vision_rows.shape[1]
    block_cols = q_weight.shape[1]
    width = q_weight.shape[0]
    image_rows = IMG_MAX * PATCH
    own_rows = q_grad.shape[0] // groups
    text_rows = own_rows - image_rows
    per_shard = proj_flat.shape[0] * 128 // block_cols
    bf16 = jnp.bfloat16

    q_own = q_grad.reshape(groups, own_rows, block_cols)
    q_image = q_own[:, :image_rows].reshape(groups * image_rows, block_cols)
    q_text = q_own[:, image_rows:].reshape(groups * text_rows, block_cols)
    image_part = contract_last(q_weight, q_image).astype(bf16)
    image_norm = lax.psum_scatter(image_part, "y", scatter_dimension=0, tiled=True)
    text_part = contract_last(q_text, q_weight).astype(bf16)
    text_norm = lax.psum_scatter(text_part, "y", scatter_dimension=0, tiled=True)

    order = jnp.arange(shards * per_shard, dtype=jnp.int32)
    row = order % per_shard
    zi = order // per_shard % nz
    xi = order // (per_shard * nz) % nx
    ci = order // (per_shard * nz * nx)
    source = ((zi * nx + xi) * nc + ci) * per_shard + row
    pick = (jnp.arange(enc_width, dtype=jnp.int32)[:, None] == source[None, :]).astype(bf16)
    vision = jnp.dot(vision_rows, pick, preferred_element_type=jnp.float32).astype(bf16)

    shard = proj_flat.reshape(per_shard, block_cols)
    over_z = spread(shard, "z").reshape(nz * per_shard, block_cols)
    over_x = spread(over_z, "x").reshape(nx * nz * per_shard, block_cols)
    proj = spread(over_x, "c").reshape(shards * per_shard, block_cols)
    embed = lax.dot_general(
        proj, vision, (((0,), (1,)), ((), ())), preferred_element_type=jnp.float32
    ).astype(bf16)

    gain_own = lax.dynamic_slice_in_dim(norm_gain, lax.axis_index("y") * block_cols, block_cols, 0)
    inputs = embed.astype(jnp.float32)
    scaled = gain_own[:, None] * image_norm.astype(jnp.float32)
    stats = jnp.stack([jnp.sum(inputs * inputs, axis=0), jnp.sum(scaled * inputs, axis=0)])
    stats = jnp.sum(spread(stats, "y").reshape(groups, 2, groups * image_rows), axis=0) / width
    inv_rms = lax.rsqrt(stats[0] + norm_eps)
    row_ids = jnp.arange(groups * image_rows, dtype=jnp.int32)
    owner_match = (row_ids // image_rows)[:, None] == jnp.arange(groups, dtype=jnp.int32)[None, :]
    counts = jnp.sum(jnp.where(owner_match, image_count[None, :], 0), axis=1)
    live = row_ids % image_rows // PATCH < counts
    image_grad = inv_rms[None, :] * scaled - inputs * (inv_rms**3 * stats[1])[None, :]
    image_grad = jnp.where(live[None, :], image_grad, 0.0).astype(bf16)
    grad_scale = 1.0 / jnp.sqrt(jnp.float32(shards * groups * image_rows))
    proj_part = (
        lax.dot_general(
            vision, image_grad, (((0,), (1,)), ((), ())), preferred_element_type=jnp.float32
        )
        * grad_scale
    )
    part = summed(proj_part.reshape(nc, nx * nz * per_shard, block_cols), "c")
    part = summed(part.reshape(nx, nz * per_shard, block_cols), "x")
    part = summed(part.reshape(nz, per_shard, block_cols), "z")
    proj_grad = part.reshape(proj_flat.shape)

    text_in = text_embeds.astype(jnp.float32)
    text_rms = lax.rsqrt(jnp.mean(text_in * text_in, axis=-1, keepdims=True) + norm_eps)
    text_scaled = norm_gain[None, :] * text_norm.astype(jnp.float32)
    inner = jnp.mean(text_scaled * text_in, axis=-1, keepdims=True)
    text_grad = (text_rms * text_scaled - text_in * text_rms**3 * inner).astype(bf16)
    return (text_grad, proj_grad)


def solution(mesh):
    finer = Mesh(mesh.devices.reshape(12, 4, 2, mesh.shape["mp"]), DP_MP)
    placed = (P(DP, None), P(DP), P(DP_MP, None), P(DP_MP, None), P(), P(None, "y"), P(DP, "y"))
    return jax.shard_map(
        body,
        mesh=finer,
        in_specs=placed,
        out_specs=(P(DP_MP, None), P(DP_MP, None)),
        check_vma=False,
    )
```

```python
import jax
import jax.numpy as jnp
from jax import lax
from jax.sharding import Mesh
from jax.sharding import PartitionSpec as P

IMG_MAX = 4
PATCH = 8
DP = ("z", "x", "c")
DP_MP = ("z", "x", "c", "y")

norm_eps = 1e-05
bf16 = jnp.bfloat16
f32 = jnp.float32


def dot(left, right, dims):
    return lax.dot_general(left, right, (dims, ((), ())), preferred_element_type=f32)


def spread(block, axis):
    n = lax.axis_size(axis)
    copies = jnp.broadcast_to(block[None], (n, *block.shape))
    return lax.all_to_all(copies, axis, split_axis=0, concat_axis=0, tiled=True)


def summed(blocks, axis):
    parts = lax.all_to_all(blocks.astype(bf16), axis, split_axis=0, concat_axis=0, tiled=True)
    return jnp.sum(parts.astype(f32), axis=0)


def gathered(shard):
    for axis in ("z", "x", "c"):
        parts = spread(shard, axis)
        shard = parts.reshape(-1, shard.shape[-1])
    return shard


def body(vision_rows, image_count, proj_flat, text_embeds, norm_gain, q_weight, q_grad):
    groups = lax.axis_size("y")
    member = lax.axis_index("y")
    nz, nx, nc = (lax.axis_size(a) for a in DP)
    shards = nz * nx * nc
    enc = vision_rows.shape[1]
    cols = q_weight.shape[1]
    width = q_weight.shape[0]
    image_rows = IMG_MAX * PATCH
    own_rows = q_grad.shape[0] // groups
    text_rows = own_rows - image_rows
    per_shard = proj_flat.shape[0] * 128 // cols
    enc_block = enc // groups

    q_own = q_grad.reshape(groups, own_rows, cols)
    q_text = q_own[:, image_rows:].reshape(groups * text_rows, cols)
    text_part = dot(q_text, q_weight, ((1,), (1,))).astype(bf16)
    text_norm = lax.psum_scatter(text_part, "y", scatter_dimension=0, tiled=True)

    shard = proj_flat.reshape(per_shard, cols)
    gain_blocks = norm_gain.reshape(groups, 1, cols)
    group_rows = (spread(shard, "y").astype(f32) * gain_blocks).astype(bf16)
    through = dot(group_rows, q_weight.reshape(groups, cols, cols), ((0, 2), (0, 1))).astype(bf16)
    proj = gathered(shard)
    through = gathered(through)

    order = jnp.arange(shards * per_shard, dtype=jnp.int32)
    row = order % per_shard
    zi = order // per_shard % nz
    xi = order // (per_shard * nz) % nx
    ci = order // (per_shard * nz * nx)
    source = ((zi * nx + xi) * nc + ci) * per_shard + row
    pick = (jnp.arange(enc, dtype=jnp.int32)[:, None] == source[None, :]).astype(bf16)
    vision = dot(vision_rows, pick, ((1,), (0,))).astype(bf16)
    proj_rows = dot(pick, proj, ((1,), (0,))).astype(bf16)

    q_image = q_own[:, :image_rows].reshape(groups * image_rows, cols).T.astype(f32)
    embed = dot(proj, vision, ((0,), (1,)))
    pulled = dot(through, vision, ((0,), (1,)))
    stats = jnp.stack([jnp.sum(embed * embed, axis=0), jnp.sum(q_image * pulled, axis=0)])
    stats = jnp.sum(spread(stats, "y"), axis=0) / width
    inv_rms = lax.rsqrt(stats[0] + norm_eps)
    row_ids = jnp.arange(groups * image_rows, dtype=jnp.int32)
    owner_match = (row_ids // image_rows)[:, None] == jnp.arange(groups, dtype=jnp.int32)[None, :]
    counts = jnp.sum(jnp.where(owner_match, image_count[None, :], 0), axis=1)
    live = row_ids % image_rows // PATCH < counts
    grad_scale = 1.0 / jnp.sqrt(f32(shards * groups * image_rows))
    first = jnp.where(live, inv_rms, 0.0) * grad_scale
    second = jnp.where(live, inv_rms**3 * stats[1], 0.0) * grad_scale

    vision_block = lax.dynamic_slice_in_dim(vision_rows, member * enc_block, enc_block, 1)
    right = jnp.concatenate(
        [
            (q_image * first[None, :]).astype(bf16),
            (vision_block.T.astype(f32) * second[None, :]).astype(bf16),
        ],
        axis=0,
    )
    part = dot(vision, right, ((0,), (1,)))
    part = summed(part.reshape(nc, nx * nz * per_shard, cols + enc_block), "c")
    part = summed(part.reshape(nx, nz * per_shard, cols + enc_block), "x")
    part = summed(part.reshape(nz, per_shard, cols + enc_block), "z").astype(bf16)
    through_weight = dot(part[:, :cols], q_weight, ((1,), (1,))).astype(bf16)
    through_weight = through_weight.reshape(per_shard, groups, cols).transpose(1, 0, 2)
    moments = jnp.broadcast_to(part[None, :, cols:], (groups, per_shard, enc_block))
    parts = lax.all_to_all(
        jnp.concatenate([through_weight, moments], axis=2), "y", split_axis=0, concat_axis=0, tiled=True
    )
    gain_own = lax.dynamic_slice_in_dim(norm_gain, member * cols, cols, 0)
    plain = jnp.sum(parts[:, :, :cols].astype(f32), axis=0) * gain_own[None, :]
    radial = dot(parts[:, :, cols:], proj_rows.reshape(groups, enc_block, cols), ((0, 2), (0, 1)))
    proj_grad = (plain - radial).reshape(proj_flat.shape)

    text_in = text_embeds.astype(f32)
    text_rms = lax.rsqrt(jnp.mean(text_in * text_in, axis=-1, keepdims=True) + norm_eps)
    text_scaled = norm_gain[None, :] * text_norm.astype(f32)
    inner = jnp.mean(text_scaled * text_in, axis=-1, keepdims=True)
    text_grad = (text_rms * text_scaled - text_in * text_rms**3 * inner).astype(bf16)
    return (text_grad, proj_grad)


def solution(mesh):
    finer = Mesh(mesh.devices.reshape(12, 4, 2, mesh.shape["mp"]), DP_MP)
    placed = (P(DP, None), P(DP), P(DP_MP, None), P(DP_MP, None), P(), P(None, "y"), P(DP, "y"))
    return jax.shard_map(
        body,
        mesh=finer,
        in_specs=placed,
        out_specs=(P(DP_MP, None), P(DP_MP, None)),
        check_vma=False,
    )
```

```python
import jax
import jax.numpy as jnp
from jax import lax
from jax.sharding import Mesh
from jax.sharding import PartitionSpec as P


IMG_MAX = 4
PATCH = 8
DP = ("z", "x", "c")
DP_MP = ("z", "x", "c", "y")

norm_eps = 1e-05
bf16 = jnp.bfloat16
f32 = jnp.float32


def dot(left, right, left_dim, right_dim):
    return lax.dot_general(
        left, right, (((left_dim,), (right_dim,)), ((), ())), preferred_element_type=f32
    )


def spread(block, axis):
    n = lax.axis_size(axis)
    copies = jnp.broadcast_to(block[None], (n, *block.shape))
    return lax.all_to_all(copies, axis, split_axis=0, concat_axis=0, tiled=True)


def summed(blocks, axis):
    parts = lax.all_to_all(blocks.astype(bf16), axis, split_axis=0, concat_axis=0, tiled=True)
    return jnp.sum(parts.astype(f32), axis=0)


def swapped(block):
    return lax.ppermute(block, "c", [(0, 1), (1, 0)])


def shift(value, axis, by):
    n = lax.axis_size(axis)
    return lax.ppermute(value, axis, [(i, (i + by) % n) for i in range(n)])


def column_sum(part, axis):
    n = lax.axis_size(axis)
    me = lax.axis_index(axis)
    size = part.shape[0] // n
    half = size // 2

    def chunk(k, start=0, count=size):
        return lax.dynamic_slice_in_dim(part, (me + k) % n * size + start, count, 0)

    near_up = shift(jnp.concatenate([chunk(3), chunk(1)], axis=0), axis, 1)
    near_down = shift(jnp.concatenate([chunk(-3), chunk(-1)], axis=0), axis, -1)
    far_up = shift(chunk(4, 0, half), axis, 2)
    far_down = shift(chunk(4, half, half), axis, -2)
    rest = jnp.zeros((half, part.shape[1]), f32)
    up = jnp.concatenate([far_up.astype(f32), rest], axis=0)
    up = (up + chunk(2).astype(f32) + near_up[:size].astype(f32)).astype(part.dtype)
    up = shift(up, axis, 2)
    down = jnp.concatenate([rest, far_down.astype(f32)], axis=0)
    down = (down + chunk(-2).astype(f32) + near_down[:size].astype(f32)).astype(part.dtype)
    down = shift(down, axis, -2)
    near = chunk(0).astype(f32) + near_up[size:].astype(f32) + near_down[size:].astype(f32)
    return near + up.astype(f32) + down.astype(f32)


def compute(vision_rows, image_count, proj_flat, text_embeds, norm_gain, q_weight, q_grad):
    groups = lax.axis_size("y")
    member = lax.axis_index("y")
    nz, nx, nc = (lax.axis_size(a) for a in DP)
    shards = nz * nx * nc
    enc = vision_rows.shape[1]
    cols = q_weight.shape[1]
    width = q_weight.shape[0]
    image_rows = IMG_MAX * PATCH
    own_rows = q_grad.shape[0] // groups
    text_rows = own_rows - image_rows
    per_shard = proj_flat.shape[0] * 128 // cols
    half = nx * nz * per_shard

    rows = spread(proj_flat.reshape(per_shard, cols), "z")
    rows = rows.reshape(nz * per_shard, cols)
    rows = spread(rows, "x")
    rows = rows.reshape(half, cols)
    proj = jnp.concatenate([rows, swapped(rows)], axis=0)

    q_own = q_grad.reshape(groups, own_rows, cols)
    q_image = q_own[:, :image_rows].reshape(groups * image_rows, cols)
    q_text = q_own[:, image_rows:].reshape(groups * text_rows, cols)
    image_part = dot(q_weight, q_image, 1, 1).astype(bf16)
    image_norm = column_sum(image_part, "y")
    text_part = dot(q_text, q_weight, 1, 1).astype(bf16)
    text_norm = lax.psum_scatter(text_part, "y", scatter_dimension=0, tiled=True)

    order = jnp.arange(shards * per_shard, dtype=jnp.int32)
    row = order % per_shard
    zi = order // per_shard % nz
    xi = order // (per_shard * nz) % nx
    ci = (order // half + lax.axis_index("c")) % nc
    source = ((zi * nx + xi) * nc + ci) * per_shard + row
    pick = (jnp.arange(enc, dtype=jnp.int32)[:, None] == source[None, :]).astype(bf16)
    vision = dot(vision_rows, pick, 1, 0).astype(bf16)
    embed = dot(proj, vision, 0, 1).astype(bf16)
    squares = jnp.sum(jnp.square(embed.astype(f32)), axis=0)
    embed, squares = lax.optimization_barrier((embed, squares))
    inputs = embed.astype(f32)

    gain_own = lax.dynamic_slice_in_dim(norm_gain, member * cols, cols, 0)
    scaled = gain_own[:, None] * image_norm
    stats = jnp.stack([squares, jnp.sum(scaled * inputs, axis=0)])
    stats = spread(stats, "y")
    stats = jnp.sum(stats, axis=0) / width
    inv_rms = lax.rsqrt(stats[0] + norm_eps)
    row_ids = jnp.arange(groups * image_rows, dtype=jnp.int32)
    owner_match = (row_ids // image_rows)[:, None] == jnp.arange(groups, dtype=jnp.int32)[None, :]
    counts = jnp.sum(jnp.where(owner_match, image_count[None, :], 0), axis=1)
    live = row_ids % image_rows // PATCH < counts
    image_grad = inv_rms[None, :] * scaled - inputs * (inv_rms**3 * stats[1])[None, :]
    grad_scale = 1.0 / jnp.sqrt(f32(shards * groups * image_rows))
    image_grad = jnp.where(live[None, :], image_grad * grad_scale, 0.0).astype(bf16)
    other = dot(vision[:, half:], image_grad, 0, 1).astype(bf16)
    other = swapped(other)
    part = dot(vision[:, :half], image_grad, 0, 1) + other.astype(f32)
    part = summed(part.reshape(nx, nz * per_shard, cols), "x")
    part = summed(part.reshape(nz, per_shard, cols), "z")
    proj_grad = part.reshape(proj_flat.shape)

    text_in = text_embeds.astype(f32)
    text_rms = lax.rsqrt(jnp.mean(text_in * text_in, axis=-1, keepdims=True) + norm_eps)
    text_scaled = norm_gain[None, :] * text_norm.astype(f32)
    inner = jnp.mean(text_scaled * text_in, axis=-1, keepdims=True)
    text_grad = (text_rms * text_scaled - text_in * text_rms**3 * inner).astype(bf16)
    return (text_grad, proj_grad)


def solution(mesh):
    finer = Mesh(mesh.devices.reshape(12, 4, 2, mesh.shape["mp"]), DP_MP)
    placed = (P(DP, None), P(DP), P(DP_MP, None), P(DP_MP, None), P(), P(None, "y"), P(DP, "y"))
    return jax.shard_map(
        compute,
        mesh=finer,
        in_specs=placed,
        out_specs=(P(DP_MP, None), P(DP_MP, None)),
        check_vma=False,
    )
```

```python
import jax
import jax.numpy as jnp
from jax import lax
from jax.sharding import Mesh
from jax.sharding import PartitionSpec as P


IMG_MAX = 4
PATCH = 8
DP = ("z", "x", "c")
DP_MP = ("z", "x", "c", "y")

norm_eps = 1e-05
bf16 = jnp.bfloat16
f32 = jnp.float32


def dot(left, right, left_dim, right_dim):
    return lax.dot_general(
        left, right, (((left_dim,), (right_dim,)), ((), ())), preferred_element_type=f32
    )


def spread(block, axis):
    n = lax.axis_size(axis)
    copies = jnp.broadcast_to(block[None], (n, *block.shape))
    return lax.all_to_all(copies, axis, split_axis=0, concat_axis=0, tiled=True)


def summed(blocks, axis):
    parts = lax.all_to_all(blocks.astype(bf16), axis, split_axis=0, concat_axis=0, tiled=True)
    return jnp.sum(parts.astype(f32), axis=0)


def swapped(block):
    return lax.ppermute(block, "c", [(0, 1), (1, 0)])


def shift(value, axis, by):
    n = lax.axis_size(axis)
    return lax.ppermute(value, axis, [(i, (i + by) % n) for i in range(n)])


def column_sum(part, axis):
    n = lax.axis_size(axis)
    me = lax.axis_index(axis)
    size = part.shape[0] // n
    half = size // 2

    def chunk(k, start=0, count=size):
        return lax.dynamic_slice_in_dim(part, (me + k) % n * size + start, count, 0)

    near_up = shift(jnp.concatenate([chunk(3), chunk(1)], axis=0), axis, 1)
    near_down = shift(jnp.concatenate([chunk(-3), chunk(-1)], axis=0), axis, -1)
    far_up = shift(chunk(4, 0, half), axis, 2)
    far_down = shift(chunk(4, half, half), axis, -2)
    rest = jnp.zeros((half, part.shape[1]), f32)
    up = jnp.concatenate([far_up.astype(f32), rest], axis=0)
    up = (up + chunk(2).astype(f32) + near_up[:size].astype(f32)).astype(part.dtype)
    up = shift(up, axis, 2)
    down = jnp.concatenate([rest, far_down.astype(f32)], axis=0)
    down = (down + chunk(-2).astype(f32) + near_down[:size].astype(f32)).astype(part.dtype)
    down = shift(down, axis, -2)
    near = chunk(0).astype(f32) + near_up[size:].astype(f32) + near_down[size:].astype(f32)
    return near + up.astype(f32) + down.astype(f32)


def compute(vision_rows, image_count, proj_flat, text_embeds, norm_gain, q_weight, q_grad):
    groups = lax.axis_size("y")
    member = lax.axis_index("y")
    nz, nx, nc = (lax.axis_size(a) for a in DP)
    shards = nz * nx * nc
    enc = vision_rows.shape[1]
    cols = q_weight.shape[1]
    width = q_weight.shape[0]
    image_rows = IMG_MAX * PATCH
    own_rows = q_grad.shape[0] // groups
    text_rows = own_rows - image_rows
    per_shard = proj_flat.shape[0] * 128 // cols
    half = nx * nz * per_shard

    rows = spread(proj_flat, "z")
    rows = rows.reshape(nz * per_shard, cols)
    rows = spread(rows, "x")
    rows = rows.reshape(half, cols)
    proj = jnp.concatenate([rows, swapped(rows)], axis=0)

    q_own = q_grad.reshape(groups, own_rows, cols)
    q_image = q_own[:, :image_rows].reshape(groups * image_rows, cols)
    q_text = q_own[:, image_rows:].reshape(groups * text_rows, cols)
    image_part = dot(q_weight, q_image, 1, 1).astype(bf16)
    image_part, q_text = lax.optimization_barrier((image_part, q_text))
    image_norm = column_sum(image_part, "y")
    text_part = dot(q_text, q_weight, 1, 1).astype(bf16)
    text_norm = lax.psum_scatter(text_part, "y", scatter_dimension=0, tiled=True)

    order = jnp.arange(shards * per_shard, dtype=jnp.int32)
    row = order % per_shard
    zi = order // per_shard % nz
    xi = order // (per_shard * nz) % nx
    ci = (order // half + lax.axis_index("c")) % nc
    source = ((zi * nx + xi) * nc + ci) * per_shard + row
    pick = (jnp.arange(enc, dtype=jnp.int32)[:, None] == source[None, :]).astype(bf16)
    vision = dot(vision_rows, pick, 1, 0).astype(bf16)
    embed = dot(proj, vision, 0, 1).astype(bf16)
    squares = jnp.sum(jnp.square(embed.astype(f32)), axis=0)
    inputs = embed.astype(f32)

    row_ids = jnp.arange(groups * image_rows, dtype=jnp.int32)
    owner_match = (row_ids // image_rows)[:, None] == jnp.arange(groups, dtype=jnp.int32)[None, :]
    counts = jnp.sum(jnp.where(owner_match, image_count[None, :], 0), axis=1)
    live = row_ids % image_rows // PATCH < counts

    gain_own = lax.dynamic_slice_in_dim(norm_gain, member * cols, cols, 0)
    scaled = gain_own[:, None] * image_norm
    scaled = lax.optimization_barrier(scaled)
    stats = jnp.stack([squares, jnp.sum(scaled * inputs, axis=0)])
    stats = spread(stats, "y")
    stats = jnp.sum(stats, axis=0) / width
    inv_rms = lax.rsqrt(stats[0] + norm_eps)
    image_grad = inv_rms[None, :] * scaled - inputs * (inv_rms**3 * stats[1])[None, :]
    grad_scale = 1.0 / jnp.sqrt(f32(shards * groups * image_rows))
    image_grad = jnp.where(live[None, :], image_grad * grad_scale, 0.0).astype(bf16)
    other = dot(vision[:, half:], image_grad, 0, 1).astype(bf16)
    other = swapped(other)
    part = dot(vision[:, :half], image_grad, 0, 1) + other.astype(f32)
    part = summed(part.reshape(nx, nz * per_shard, cols), "x")
    proj_grad = summed(part.reshape(nz, *proj_flat.shape), "z")

    text_in = text_embeds.astype(f32)
    text_rms = lax.rsqrt(jnp.mean(text_in * text_in, axis=-1, keepdims=True) + norm_eps)
    text_scaled = norm_gain[None, :] * text_norm.astype(f32)
    inner = jnp.mean(text_scaled * text_in, axis=-1, keepdims=True)
    text_grad = (text_rms * text_scaled - text_in * text_rms**3 * inner).astype(bf16)
    return (text_grad, proj_grad)


def solution(mesh):
    finer = Mesh(mesh.devices.reshape(12, 4, 2, mesh.shape["mp"]), DP_MP)
    placed = (P(DP, None), P(DP), P(DP_MP, None), P(DP_MP, None), P(), P(None, "y"), P(DP, "y"))
    return jax.shard_map(
        compute,
        mesh=finer,
        in_specs=placed,
        out_specs=(P(DP_MP, None), P(DP_MP, None)),
        check_vma=False,
    )
```

```python
import jax
import jax.numpy as jnp
from jax import lax
from jax.sharding import Mesh
from jax.sharding import PartitionSpec as P


IMG_MAX = 4
PATCH = 8
DP = ("z", "x", "c")
DP_MP = ("z", "x", "c", "y")

norm_eps = 1e-05
bf16 = jnp.bfloat16
f32 = jnp.float32


def dot(left, right, left_dim, right_dim):
    return lax.dot_general(
        left, right, (((left_dim,), (right_dim,)), ((), ())), preferred_element_type=f32
    )


def spread(block, axis):
    n = lax.axis_size(axis)
    copies = jnp.broadcast_to(block[None], (n, *block.shape))
    return lax.all_to_all(copies, axis, split_axis=0, concat_axis=0, tiled=True)


def summed(blocks, axis):
    parts = lax.all_to_all(blocks.astype(bf16), axis, split_axis=0, concat_axis=0, tiled=True)
    return jnp.sum(parts.astype(f32), axis=0)


def swapped(block):
    return lax.ppermute(block, "c", [(0, 1), (1, 0)])


def shift(value, axis, by):
    n = lax.axis_size(axis)
    return lax.ppermute(value, axis, [(i, (i + by) % n) for i in range(n)])


def column_sum(part, axis):
    n = lax.axis_size(axis)
    me = lax.axis_index(axis)
    size = part.shape[0] // n
    half = size // 2

    def chunk(k, start=0, count=size):
        return lax.dynamic_slice_in_dim(part, (me + k) % n * size + start, count, 0)

    near_up = shift(jnp.concatenate([chunk(3), chunk(1)], axis=0), axis, 1)
    near_down = shift(jnp.concatenate([chunk(-3), chunk(-1)], axis=0), axis, -1)
    far_up = shift(chunk(4, 0, half), axis, 2)
    far_down = shift(chunk(4, half, half), axis, -2)
    rest = jnp.zeros((half, part.shape[1]), f32)
    up = jnp.concatenate([far_up.astype(f32), rest], axis=0)
    up = (up + chunk(2).astype(f32) + near_up[:size].astype(f32)).astype(part.dtype)
    up = shift(up, axis, 2)
    far_down, near_down, part = lax.optimization_barrier((far_down, near_down, part))
    down = jnp.concatenate([rest, far_down.astype(f32)], axis=0)
    down = (down + chunk(-2).astype(f32) + near_down[:size].astype(f32)).astype(part.dtype)
    down = shift(down, axis, -2)
    near = chunk(0).astype(f32) + near_up[size:].astype(f32) + near_down[size:].astype(f32)
    return near + up.astype(f32) + down.astype(f32)


def compute(vision_rows, image_count, proj_flat, text_embeds, norm_gain, q_weight, q_grad):
    groups = lax.axis_size("y")
    member = lax.axis_index("y")
    nz, nx, nc = (lax.axis_size(a) for a in DP)
    shards = nz * nx * nc
    enc = vision_rows.shape[1]
    cols = q_weight.shape[1]
    width = q_weight.shape[0]
    image_rows = IMG_MAX * PATCH
    own_rows = q_grad.shape[0] // groups
    text_rows = own_rows - image_rows
    per_shard = proj_flat.shape[0] * 128 // cols
    half = nx * nz * per_shard

    rows = spread(proj_flat, "z")
    rows = rows.reshape(nz * per_shard, cols)
    rows = spread(rows, "x")
    rows = rows.reshape(half, cols)
    other_rows = swapped(rows)

    q_own = q_grad.reshape(groups, own_rows, cols)
    q_image = q_own[:, :image_rows].reshape(groups * image_rows, cols)
    q_text = q_own[:, image_rows:].reshape(groups * text_rows, cols)
    image_part = dot(q_weight, q_image, 1, 1).astype(bf16)
    image_part, q_text = lax.optimization_barrier((image_part, q_text))
    image_norm = column_sum(image_part, "y")
    text_part = dot(q_text, q_weight, 1, 1).astype(bf16)
    text_norm = lax.psum_scatter(text_part, "y", scatter_dimension=0, tiled=True)

    order = jnp.arange(shards * per_shard, dtype=jnp.int32)
    row = order % per_shard
    zi = order // per_shard % nz
    xi = order // (per_shard * nz) % nx
    ci = (order // half + lax.axis_index("c")) % nc
    source = ((zi * nx + xi) * nc + ci) * per_shard + row
    pick = (jnp.arange(enc, dtype=jnp.int32)[:, None] == source[None, :]).astype(bf16)
    vision = dot(vision_rows, pick, 1, 0).astype(bf16)
    embed_own = dot(rows, vision[:, :half], 0, 1)
    embed_own = lax.optimization_barrier(embed_own)
    embed = (embed_own + dot(other_rows, vision[:, half:], 0, 1)).astype(bf16)
    squares = jnp.sum(jnp.square(embed.astype(f32)), axis=0)
    inputs = embed.astype(f32)

    row_ids = jnp.arange(groups * image_rows, dtype=jnp.int32)
    owner_match = (row_ids // image_rows)[:, None] == jnp.arange(groups, dtype=jnp.int32)[None, :]
    counts = jnp.sum(jnp.where(owner_match, image_count[None, :], 0), axis=1)
    live = row_ids % image_rows // PATCH < counts

    gain_own = lax.dynamic_slice_in_dim(norm_gain, member * cols, cols, 0)
    scaled = gain_own[:, None] * image_norm
    scaled = lax.optimization_barrier(scaled)
    stats = jnp.stack([squares, jnp.sum(scaled * inputs, axis=0)])
    stats = spread(stats, "y")
    stats = jnp.sum(stats, axis=0) / width
    inv_rms = lax.rsqrt(stats[0] + norm_eps)
    image_grad = inv_rms[None, :] * scaled - inputs * (inv_rms**3 * stats[1])[None, :]
    grad_scale = 1.0 / jnp.sqrt(f32(shards * groups * image_rows))
    image_grad = jnp.where(live[None, :], image_grad * grad_scale, 0.0).astype(bf16)
    other = dot(vision[:, half:], image_grad, 0, 1).astype(bf16)
    other = swapped(other)
    part = dot(vision[:, :half], image_grad, 0, 1) + other.astype(f32)
    part = summed(part.reshape(nx, nz * per_shard, cols), "x")
    proj_grad = summed(part.reshape(nz, *proj_flat.shape), "z")

    text_in = text_embeds.astype(f32)
    text_rms = lax.rsqrt(jnp.mean(text_in * text_in, axis=-1, keepdims=True) + norm_eps)
    text_scaled = norm_gain[None, :] * text_norm.astype(f32)
    inner = jnp.mean(text_scaled * text_in, axis=-1, keepdims=True)
    text_grad = (text_rms * text_scaled - text_in * text_rms**3 * inner).astype(bf16)
    return (text_grad, proj_grad)


def solution(mesh):
    finer = Mesh(mesh.devices.reshape(12, 4, 2, mesh.shape["mp"]), DP_MP)
    placed = (P(DP, None), P(DP), P(DP_MP, None), P(DP_MP, None), P(), P(None, "y"), P(DP, "y"))
    return jax.shard_map(
        compute,
        mesh=finer,
        in_specs=placed,
        out_specs=(P(DP_MP, None), P(DP_MP, None)),
        check_vma=False,
    )
```
